256 devices in a mesh: tm: 32 (over x_hi, z, core), freq: 8 (over x_lo, y).
Axes of the slice: x: 4 (x_hi: 2, x_lo: 2; x = x_hi * 2 + x_lo), y: 4, z: 8, core: 2. Of those that a mesh axis runs over, the one named last changes fastest.
Arguments:
- strengths: bfloat16 [2, 8, 256, 65536], P(None, 'freq', None, 'tm'), may hold values from -6 to 6
- sample_cell: int32 [65536], P('tm'), may hold values from 0 to 32767, as said below
- sample_frac: float32 [65536], P('tm'), may hold values from 0 to 1
Outputs:
- spectra: float32 [2, 8, 256, 8, 32, 128], P(None, None, 'tm', 'freq')
The draws below stay inside these ranges and needn't reach their ends.
Inputs may be any that keep to these rules, and one draw needn't show every extreme that they name: `sample_cell`: the samples of the i-th aligned block of 2048 samples lie in cells i * 1024 to (i + 1) * 1024 - 1; in every block the first sample lies in the first of these cells and the second sample in the last.
All inputs are finite; a program needn't handle non-finite values.
Results may differ from the reference program's by a relative error of at most 0.0037.
Values may be sent and summed in bfloat16 or wider, within the bound.
A program may use at most 128 MiB of HBM per device.

```python
import math
import jax
import jax.numpy as jnp
from jax import lax

TAPS = 8
FGROUPS = 8
CHG = 256
GRID_DEV = 1024
SAMP_DEV = 2048
FFT_LO = 32
FFT_HI = 128
FFTLEN = 4096
SAMPLES = 65536
CELLS = 32768
FRAMES = 8


def draw_sample_cell(key, part):
    offsets = jax.random.randint(key, (SAMPLES,), 0, GRID_DEV)
    within = jnp.arange(SAMPLES) % SAMP_DEV
    offsets = jnp.where(within == 0, 0, jnp.where(within == 1, GRID_DEV - 1, offsets))
    blocks = jnp.arange(SAMPLES) // SAMP_DEV
    return (blocks * GRID_DEV + offsets).astype(jnp.int32)


def levels(rng, dims, cuts, least, largest):
    gain, own = 1.0, jax.random.fold_in(rng, 6)
    for dim, blocks in cuts:
        heights = jnp.exp(jax.random.uniform(jax.random.fold_in(own, dim), (blocks,), jnp.float32, least / len(cuts), largest / len(cuts)))
        gain = gain * jnp.repeat(heights, dims[dim] // blocks).reshape([-1 if axis == dim else 1 for axis in range(len(dims))])
    return gain


def scatter_about(key, dims, scale, reach, shards=(), dtype=jnp.bfloat16):
    factor_of = levels(key, dims, shards, -0.22, 0.18) if shards else 1.0
    drawn = jax.random.normal(key, dims, jnp.float32) * scale * factor_of
    return jnp.minimum(jnp.maximum(drawn, -reach), reach).astype(dtype)


def setup_inputs(seed: int = 0) -> dict:
    splits = jax.random.split(jax.random.key(seed), 4)
    return {
        "strengths": scatter_about(splits[0], (2, FGROUPS, CHG, SAMPLES), 1.0, 6.0, ((1, 8), (3, 32))),
        "sample_cell": draw_sample_cell(jax.random.fold_in(splits[3], 71), 0),
        "sample_frac": jnp.clip(1.0 * jax.random.uniform(splits[2], (SAMPLES,), jnp.float32) ** levels(splits[2], (SAMPLES,), ((0, 32),), -0.2, 0.2), 0.0, 1.0),
    }


sharpness = 0.3

def one_group(group_strengths, sample_cell, sample_frac):
    values = group_strengths.astype(jnp.float32)
    accumulated = jnp.zeros((2, CHG, CELLS), jnp.float32)
    for tap_index in range(TAPS):
        shifted = jnp.float32(tap_index) - float(TAPS // 2 - 1) - sample_frac
        weight_row = lax.optimization_barrier(jnp.exp(-sharpness * (shifted * shifted)).astype(jnp.bfloat16)).astype(jnp.float32)
        target = ((sample_cell + (tap_index - (TAPS // 2 - 1))) % CELLS).astype(jnp.int32)
        accumulated = accumulated.at[:, :, target].add(values * weight_row)
    rounded = lax.optimization_barrier(accumulated.astype(jnp.bfloat16)).astype(jnp.float32)
    framed = rounded.reshape(2, CHG, FRAMES, FFTLEN)
    transform = jnp.fft.fft(framed[0] + 1j * framed[1], axis=-1) * (1.0 / math.sqrt(FFTLEN))
    parts = jnp.stack([jnp.real(transform), jnp.imag(transform)]).astype(jnp.float32)
    digits = parts.reshape(2, CHG, FRAMES, FFT_HI, FFT_LO)
    return jnp.swapaxes(digits, -1, -2)

def reference(strengths, sample_cell, sample_frac):
    by_group = jnp.moveaxis(strengths, 1, 0)
    result = lax.map(lambda group_strengths: one_group(group_strengths, sample_cell, sample_frac), by_group)
    return jnp.moveaxis(result, 0, 1)
```

```python
import math

import jax
import jax.numpy as jnp
import numpy as np
from jax import lax
from jax.experimental import pallas as pl
from jax.experimental.pallas import tpu as pltpu
from jax.sharding import PartitionSpec as P

TAPS = 8
GRID_DEV = 1024
FFT_LO = 32
FFT_HI = 128
FFTLEN = 4096
MESH = pl.DeviceIdType.MESH

sharpness = 0.3

CHUNKS = 4
CHUNK = GRID_DEV // CHUNKS
TILE = 16


def destination(step, block):
    ring, inner = step // 4, step % 4
    shift = ((ring + 1) // 2) * (2 * (ring % 2) - 1)
    half = (block // 16 + inner // 2) % 2
    return half * 16 + ((block // 2) % 8 + shift + 8) % 8 * 2 + (block + inner) % 2


def spread_kernel(
    strength_hbm,
    cell_ref,
    frac_ref,
    received,
    strength,
    window,
    outgoing,
    partial,
    halo,
    halo_in,
    load_sem,
    send_sem,
    recv_sem,
    halo_send_sem,
    halo_recv_sem,
):
    block = lax.axis_index("tm")
    group = lax.axis_index("freq")
    frame = block // 4
    blocks = 32
    right, left = (block + 1) % blocks, (block + blocks - 1) % blocks

    load = pltpu.make_async_copy(strength_hbm, strength, load_sem)
    load.start()

    barrier = pltpu.get_barrier_semaphore()

    def greet(i, carry):
        pl.semaphore_signal(
            barrier, inc=1, device_id=(4 * group + i // 8, i % 8), device_id_type=MESH
        )
        return carry

    lax.fori_loop(0, 32, greet, 0)
    for beside in (left, right):
        pl.semaphore_signal(barrier, inc=1, device_id=(beside, group), device_id_type=MESH)

    samples = cell_ref.shape[1]
    start = jnp.broadcast_to(
        cell_ref[...] - block * GRID_DEV + (TILE - (TAPS // 2 - 1)), (TILE, samples)
    )
    row = lax.broadcasted_iota(jnp.int32, (TILE, samples), 0)
    phase = start & (TILE - 1)
    tap = (row - phase) & (TILE - 1)
    shifted = tap.astype(jnp.float32) - float(TAPS // 2 - 1) - frac_ref[...]
    values = jnp.exp(-sharpness * (shifted * shifted))
    values = jnp.where(tap < TAPS, values, 0.0).astype(jnp.bfloat16)
    tile_of = (lax.shift_right_logical(start, 4) + jnp.where(row < phase, 1, 0)).astype(
        jnp.float32
    )
    edge = jnp.where(row < TILE // 2, float(GRID_DEV // TILE + 1), 0.0)
    nothing = jnp.zeros_like(values)
    edge_window = jnp.where(tile_of == edge, values.astype(jnp.float32), 0.0).astype(jnp.bfloat16)
    tile_of = tile_of.astype(jnp.bfloat16)

    def build(chunk):
        for i in range(CHUNK // TILE):
            q = chunk * (CHUNK // TILE) + i
            window[q * TILE : (q + 1) * TILE, :] = jnp.where(
                tile_of == jnp.bfloat16(q + 1), values, nothing
            )

    across = (((1,), (1,)), ((), ()))

    def rows():
        return strength[...].reshape(2 * strength.shape[2], samples)

    def gather(chunk):
        return lax.dot_general(
            rows(),
            window[chunk * CHUNK : (chunk + 1) * CHUNK, :],
            across,
            preferred_element_type=jnp.float32,
        )

    def round_out(chunk, total):
        channels = total.shape[0] // 2
        real = total[:channels].reshape(blocks, 8, total.shape[1])
        imag = total[channels:].reshape(blocks, 8, total.shape[1])
        outgoing[chunk] = jnp.concatenate([real, imag], axis=1).astype(jnp.bfloat16)

    def send(chunk):
        def one(step, carry):
            target = destination(step, block)
            src = outgoing.at[chunk, target]
            dst = received.at[group, block % 4, chunk]
            own = jnp.logical_and(target == block, frame == group)

            @pl.when(jnp.logical_not(own))
            def _():
                pltpu.make_async_remote_copy(
                    src_ref=src,
                    dst_ref=dst,
                    send_sem=send_sem,
                    recv_sem=recv_sem,
                    device_id=(target, frame),
                    device_id_type=MESH,
                ).start()

            @pl.when(own)
            def _():
                pltpu.make_async_copy(src, dst, recv_sem).start()

            return carry

        lax.fori_loop(0, blocks, one, 0)

    build(1)
    load.wait()
    round_out(1, gather(1))
    pl.semaphore_wait(barrier, 34)
    send(1)

    halo[...] = lax.dot_general(edge_window, rows(), across, preferred_element_type=jnp.float32)
    to_right = pltpu.make_async_remote_copy(
        src_ref=halo.at[0:8],
        dst_ref=halo_in.at[0:8],
        send_sem=halo_send_sem,
        recv_sem=halo_recv_sem,
        device_id=(right, group),
        device_id_type=MESH,
    )
    to_left = pltpu.make_async_remote_copy(
        src_ref=halo.at[8:16],
        dst_ref=halo_in.at[120:128],
        send_sem=halo_send_sem,
        recv_sem=halo_recv_sem,
        device_id=(left, group),
        device_id_type=MESH,
    )
    to_right.start()
    to_left.start()

    build(2)
    round_out(2, gather(2))
    send(2)
    build(0)
    partial[0] = gather(0)
    build(3)
    partial[1] = gather(3)
    halo_in[8:120, :] = jnp.zeros((112, halo_in.shape[1]), jnp.float32)

    pltpu.make_async_copy(halo, halo_in.at[0:16], halo_recv_sem).wait()
    beyond = halo_in[...].T
    lane = lax.broadcasted_iota(jnp.int32, beyond.shape, 1)
    none = jnp.zeros((beyond.shape[0], CHUNK - 128), jnp.float32)
    round_out(
        0, partial[0] + jnp.concatenate([jnp.where(lane < 8, beyond, 0.0), none], axis=1)
    )
    send(0)
    round_out(
        3, partial[1] + jnp.concatenate([none, jnp.where(lane >= 120, beyond, 0.0)], axis=1)
    )
    send(3)

    pltpu.make_async_copy(halo, halo_in.at[0:16], halo_send_sem).wait()
    pltpu.make_async_copy(outgoing, received, recv_sem).wait()

    @pl.when(frame == group)
    def _():
        pltpu.make_async_copy(
            outgoing.at[:, 0:31], outgoing.at[:, 0:31], send_sem
        ).wait()

    @pl.when(frame != group)
    def _():
        pltpu.make_async_copy(outgoing, outgoing, send_sem).wait()


def spread(strengths, sample_cell, sample_frac):
    channels, samples = strengths.shape[2], strengths.shape[3]
    rows = 2 * channels
    return pl.pallas_call(
        spread_kernel,
        out_shape=jax.ShapeDtypeStruct((8, 4, CHUNKS, 16, CHUNK), jnp.bfloat16),
        in_specs=[
            pl.BlockSpec(memory_space=pl.ANY),
            pl.BlockSpec(memory_space=pltpu.VMEM),
            pl.BlockSpec(memory_space=pltpu.VMEM),
        ],
        out_specs=pl.BlockSpec(memory_space=pl.ANY),
        scratch_shapes=[
            pltpu.VMEM(strengths.shape, jnp.bfloat16),
            pltpu.VMEM((GRID_DEV, samples), jnp.bfloat16),
            pltpu.VMEM((CHUNKS, 32, 16, CHUNK), jnp.bfloat16),
            pltpu.VMEM((2, rows, CHUNK), jnp.float32),
            pltpu.VMEM((16, rows), jnp.float32),
            pltpu.VMEM((128, rows), jnp.float32),
            pltpu.SemaphoreType.DMA,
            pltpu.SemaphoreType.DMA,
            pltpu.SemaphoreType.DMA,
            pltpu.SemaphoreType.DMA,
            pltpu.SemaphoreType.DMA,
        ],
        compiler_params=pltpu.CompilerParams(
            collective_id=0, has_side_effects=True, vmem_limit_bytes=48 * 1024 * 1024
        ),
    )(strengths, sample_cell.reshape(1, samples), sample_frac.reshape(1, samples))


def split_bf16(table):
    high = table.astype(jnp.bfloat16)
    low = (table - high.astype(np.float64)).astype(jnp.bfloat16)
    return high, low


def transform_tables():
    digit = np.arange(16)
    angle = 2.0 * math.pi * (digit[:, None] * digit[None, :] % 16) / 16
    cos, sin, same = np.cos(angle), np.sin(angle), np.eye(8)

    def block(part):
        return np.einsum("am,cd->camd", part, same)

    first = np.zeros((2, 8, 16, 16, 2, 8))
    first[0, :, :, :, 0] = block(cos)
    first[0, :, :, :, 1] = block(sin)
    first[1, :, :, :, 0] = block(-sin)
    first[1, :, :, :, 1] = block(cos)
    first = first.reshape(256, 256)

    n = np.arange(FFT_HI)
    half_turn = 2.0 * math.pi * digit[:, None] / FFT_LO * np.ones((1, FFT_HI))
    turn = 2.0 * math.pi * np.arange(FFT_LO)[:, None] * n[None, :] / FFTLEN
    turns = np.stack(
        [
            np.cos(half_turn),
            np.sin(half_turn),
            np.cos(turn[:16]),
            np.sin(turn[:16]),
            np.cos(turn[16:]),
            np.sin(turn[16:]),
        ]
    ).astype(np.float32)

    angle = 2.0 * math.pi * (n[:, None] * n[None, :] % FFT_HI) / FFT_HI
    cos, sin = np.cos(angle), np.sin(angle)
    last = np.block([[cos, -sin], [sin, cos]]) / math.sqrt(FFTLEN)
    return split_bf16(first), turns, split_bf16(last)


def transform_kernel(data_ref, first_hi, first_lo, turns, last_hi, last_lo, out_ref):
    data = data_ref[...].reshape(256, 256)

    def dot(a, b):
        return jnp.dot(a, b, preferred_element_type=jnp.float32)

    def turned(real, imag, cos, sin):
        return real * cos + imag * sin, imag * cos - real * sin

    section = dot(first_hi[...], data) + dot(first_lo[...], data)
    section = section.reshape(2, 8, 16, 256)
    even_real, odd_real = section[0, :, :, :128], section[0, :, :, 128:]
    even_imag, odd_imag = section[1, :, :, :128], section[1, :, :, 128:]
    odd_real, odd_imag = turned(odd_real, odd_imag, turns[0], turns[1])
    halves = (
        turned(even_real + odd_real, even_imag + odd_imag, turns[2], turns[3]),
        turned(even_real - odd_real, even_imag - odd_imag, turns[4], turns[5]),
    )
    for half, (real, imag) in enumerate(halves):
        both = jnp.concatenate([real.reshape(128, 128), imag.reshape(128, 128)], axis=1)
        high = both.astype(jnp.bfloat16)
        low = (both - high.astype(jnp.float32)).astype(jnp.bfloat16)
        result = dot(high, last_hi[...]) + dot(low, last_hi[...]) + dot(high, last_lo[...])
        for part in range(2):
            out_ref[part, 0, :, 0, half * 16 : half * 16 + 16, :] = result[
                :, part * 128 : (part + 1) * 128
            ].reshape(8, 16, 128)


def transform(received):
    (first_hi, first_lo), turns, (last_hi, last_lo) = transform_tables()
    table = pl.BlockSpec((256, 256), lambda g: (0, 0))
    return pl.pallas_call(
        transform_kernel,
        grid=(8,),
        out_shape=jax.ShapeDtypeStruct((2, 8, 8, 1, FFT_LO, FFT_HI), jnp.float32),
        in_specs=[
            pl.BlockSpec((1, 4, CHUNKS, 16, CHUNK), lambda g: (g, 0, 0, 0, 0)),
            table,
            table,
            pl.BlockSpec((6, 16, 128), lambda g: (0, 0, 0)),
            table,
            table,
        ],
        out_specs=pl.BlockSpec((2, 1, 8, 1, FFT_LO, FFT_HI), lambda g: (0, g, 0, 0, 0, 0)),
    )(received, first_hi, first_lo, turns, last_hi, last_lo)


def shards(strengths, sample_cell, sample_frac):
    return transform(spread(strengths, sample_cell, sample_frac))


def solution(mesh):
    placed = (P(None, "freq", None, "tm"), P("tm"), P("tm"))
    return jax.shard_map(
        shards,
        mesh=mesh,
        in_specs=placed,
        out_specs=P(None, None, "tm", "freq", None, None),
        check_vma=False,
    )
```

```python
import math

import jax
import jax.numpy as jnp
import numpy as np
from jax import lax
from jax.experimental import pallas as pl
from jax.experimental.pallas import tpu as pltpu
from jax.sharding import PartitionSpec as P

TAPS = 8
GRID_DEV = 1024
FFT_LO = 32
FFT_HI = 128
FFTLEN = 4096
MESH = pl.DeviceIdType.MESH

sharpness = 0.3

CHUNKS = 4
CHUNK = GRID_DEV // CHUNKS
TILE = 16


def destination(step, block):
    ring, inner = step // 4, step % 4
    shift = ((ring + 1) // 2) * (2 * (ring % 2) - 1)
    half = (block // 16 + inner // 2) % 2
    return half * 16 + ((block // 2) % 8 + shift + 8) % 8 * 2 + (block + inner) % 2


def spread_kernel(
    strength_hbm,
    cell_hbm,
    frac_hbm,
    received,
    cell_ref,
    frac_ref,
    strength,
    window,
    outgoing,
    partial,
    halo,
    halo_in,
    load_sem,
    send_sem,
    recv_sem,
    halo_send_sem,
    halo_recv_sem,
):
    block = lax.axis_index("tm")
    group = lax.axis_index("freq")
    frame = block // 4
    blocks = 32
    right, left = (block + 1) % blocks, (block + blocks - 1) % blocks

    loads = [
        pltpu.make_async_copy(cell_hbm, cell_ref, load_sem.at[0]),
        pltpu.make_async_copy(frac_hbm, frac_ref, load_sem.at[1]),
        pltpu.make_async_copy(strength_hbm, strength, load_sem.at[2]),
    ]
    for load in loads:
        load.start()

    barrier = pltpu.get_barrier_semaphore()

    def greet(i, carry):
        pl.semaphore_signal(
            barrier, inc=1, device_id=(4 * group + i // 8, i % 8), device_id_type=MESH
        )
        return carry

    lax.fori_loop(0, 32, greet, 0)
    for beside in (left, right):
        pl.semaphore_signal(barrier, inc=1, device_id=(beside, group), device_id_type=MESH)

    loads[0].wait()
    loads[1].wait()
    samples = cell_ref.shape[1]
    start = jnp.broadcast_to(
        cell_ref[...] - block * GRID_DEV + (TILE - (TAPS // 2 - 1)), (TILE, samples)
    )
    row = lax.broadcasted_iota(jnp.int32, (TILE, samples), 0)
    phase = start & (TILE - 1)
    tap = (row - phase) & (TILE - 1)
    shifted = tap.astype(jnp.float32) - float(TAPS // 2 - 1) - frac_ref[...]
    values = jnp.exp(-sharpness * (shifted * shifted))
    values = jnp.where(tap < TAPS, values, 0.0).astype(jnp.bfloat16)
    tile_of = (lax.shift_right_logical(start, 4) + jnp.where(row < phase, 1, 0)).astype(
        jnp.float32
    )
    edge = jnp.where(row < TILE // 2, float(GRID_DEV // TILE + 1), 0.0)
    nothing = jnp.zeros_like(values)
    edge_window = jnp.where(tile_of == edge, values.astype(jnp.float32), 0.0).astype(jnp.bfloat16)
    tile_of = tile_of.astype(jnp.bfloat16)

    def build(chunk):
        for i in range(CHUNK // TILE):
            q = chunk * (CHUNK // TILE) + i
            window[q * TILE : (q + 1) * TILE, :] = jnp.where(
                tile_of == jnp.bfloat16(q + 1), values, nothing
            )

    across = (((1,), (1,)), ((), ()))

    def rows():
        return strength[...].reshape(2 * strength.shape[2], samples)

    def gather(chunk):
        return lax.dot_general(
            rows(),
            window[chunk * CHUNK : (chunk + 1) * CHUNK, :],
            across,
            preferred_element_type=jnp.float32,
        )

    def round_out(chunk, total):
        channels = total.shape[0] // 2
        real = total[:channels].reshape(blocks, 8, total.shape[1])
        imag = total[channels:].reshape(blocks, 8, total.shape[1])
        outgoing[chunk] = jnp.concatenate([real, imag], axis=1).astype(jnp.bfloat16)

    def send(chunk):
        def one(step, carry):
            target = destination(step, block)
            src = outgoing.at[chunk, target]
            dst = received.at[group, block % 4, chunk]
            own = jnp.logical_and(target == block, frame == group)

            @pl.when(jnp.logical_not(own))
            def _():
                pltpu.make_async_remote_copy(
                    src_ref=src,
                    dst_ref=dst,
                    send_sem=send_sem,
                    recv_sem=recv_sem,
                    device_id=(target, frame),
                    device_id_type=MESH,
                ).start()

            @pl.when(own)
            def _():
                pltpu.make_async_copy(src, dst, recv_sem).start()

            return carry

        lax.fori_loop(0, blocks, one, 0)

    build(1)
    loads[2].wait()
    round_out(1, gather(1))
    pl.semaphore_wait(barrier, 34)
    send(1)

    halo[...] = lax.dot_general(edge_window, rows(), across, preferred_element_type=jnp.float32)
    to_right = pltpu.make_async_remote_copy(
        src_ref=halo.at[0:8],
        dst_ref=halo_in.at[0:8],
        send_sem=halo_send_sem,
        recv_sem=halo_recv_sem,
        device_id=(right, group),
        device_id_type=MESH,
    )
    to_left = pltpu.make_async_remote_copy(
        src_ref=halo.at[8:16],
        dst_ref=halo_in.at[120:128],
        send_sem=halo_send_sem,
        recv_sem=halo_recv_sem,
        device_id=(left, group),
        device_id_type=MESH,
    )
    to_right.start()
    to_left.start()

    build(2)
    round_out(2, gather(2))
    send(2)
    build(0)
    partial[0] = gather(0)
    build(3)
    partial[1] = gather(3)
    halo_in[8:120, :] = jnp.zeros((112, halo_in.shape[1]), jnp.float32)

    pltpu.make_async_copy(halo, halo_in.at[0:16], halo_recv_sem).wait()
    beyond = halo_in[...].T
    lane = lax.broadcasted_iota(jnp.int32, beyond.shape, 1)
    none = jnp.zeros((beyond.shape[0], CHUNK - 128), jnp.float32)
    round_out(
        0, partial[0] + jnp.concatenate([jnp.where(lane < 8, beyond, 0.0), none], axis=1)
    )
    send(0)
    round_out(
        3, partial[1] + jnp.concatenate([none, jnp.where(lane >= 120, beyond, 0.0)], axis=1)
    )
    send(3)

    pltpu.make_async_copy(halo, halo_in.at[0:16], halo_send_sem).wait()
    pltpu.make_async_copy(outgoing, received, recv_sem).wait()

    @pl.when(frame == group)
    def _():
        pltpu.make_async_copy(
            outgoing.at[:, 0:31], outgoing.at[:, 0:31], send_sem
        ).wait()

    @pl.when(frame != group)
    def _():
        pltpu.make_async_copy(outgoing, outgoing, send_sem).wait()


def spread(strengths, sample_cell, sample_frac):
    channels, samples = strengths.shape[2], strengths.shape[3]
    rows = 2 * channels
    return pl.pallas_call(
        spread_kernel,
        out_shape=jax.ShapeDtypeStruct((8, 4, CHUNKS, 16, CHUNK), jnp.bfloat16),
        in_specs=[pl.BlockSpec(memory_space=pltpu.HBM)] * 3,
        out_specs=pl.BlockSpec(memory_space=pltpu.VMEM),
        scratch_shapes=[
            pltpu.VMEM((1, samples), jnp.int32),
            pltpu.VMEM((1, samples), jnp.float32),
            pltpu.VMEM(strengths.shape, jnp.bfloat16),
            pltpu.VMEM((GRID_DEV, samples), jnp.bfloat16),
            pltpu.VMEM((CHUNKS, 32, 16, CHUNK), jnp.bfloat16),
            pltpu.VMEM((2, rows, CHUNK), jnp.float32),
            pltpu.VMEM((16, rows), jnp.float32),
            pltpu.VMEM((128, rows), jnp.float32),
            pltpu.SemaphoreType.DMA((3,)),
            pltpu.SemaphoreType.DMA,
            pltpu.SemaphoreType.DMA,
            pltpu.SemaphoreType.DMA,
            pltpu.SemaphoreType.DMA,
        ],
        compiler_params=pltpu.CompilerParams(
            collective_id=0, has_side_effects=True, vmem_limit_bytes=48 * 1024 * 1024
        ),
    )(
        *(
            pltpu.with_memory_space_constraint(x, pltpu.HBM)
            for x in (strengths, sample_cell.reshape(1, samples), sample_frac.reshape(1, samples))
        )
    )


def split_bf16(table):
    high = table.astype(jnp.bfloat16)
    low = (table - high.astype(np.float64)).astype(jnp.bfloat16)
    return high, low


def transform_tables():
    digit = np.arange(16)
    angle = 2.0 * math.pi * (digit[:, None] * digit[None, :] % 16) / 16
    cos, sin, same = np.cos(angle), np.sin(angle), np.eye(8)

    def block(part):
        return np.einsum("am,cd->camd", part, same)

    first = np.zeros((2, 8, 16, 16, 2, 8))
    first[0, :, :, :, 0] = block(cos)
    first[0, :, :, :, 1] = block(sin)
    first[1, :, :, :, 0] = block(-sin)
    first[1, :, :, :, 1] = block(cos)
    first = first.reshape(256, 256)

    n = np.arange(FFT_HI)
    half_turn = 2.0 * math.pi * digit[:, None] / FFT_LO * np.ones((1, FFT_HI))
    turn = 2.0 * math.pi * np.arange(FFT_LO)[:, None] * n[None, :] / FFTLEN
    turns = np.stack(
        [
            np.cos(half_turn),
            np.sin(half_turn),
            np.cos(turn[:16]),
            np.sin(turn[:16]),
            np.cos(turn[16:]),
            np.sin(turn[16:]),
        ]
    ).astype(np.float32)

    angle = 2.0 * math.pi * (n[:, None] * n[None, :] % FFT_HI) / FFT_HI
    cos, sin = np.cos(angle), np.sin(angle)
    last = np.block([[cos, -sin], [sin, cos]]) / math.sqrt(FFTLEN)
    return split_bf16(first), turns, split_bf16(last)


def transform_kernel(data_ref, first_hi, first_lo, turns, last_hi, last_lo, out_hbm, out, sem):
    def dot(a, b):
        return jnp.dot(a, b, preferred_element_type=jnp.float32)

    def turned(real, imag, cos, sin):
        return real * cos + imag * sin, imag * cos - real * sin

    def store(group):
        return pltpu.make_async_copy(out.at[group], out_hbm.at[:, group, :, 0], sem)

    groups = data_ref.shape[0]
    for group in range(groups):
        data = data_ref[group].reshape(256, 256)
        section = dot(first_hi[...], data) + dot(first_lo[...], data)
        section = section.reshape(2, 8, 16, 256)
        even_real, odd_real = section[0, :, :, :128], section[0, :, :, 128:]
        even_imag, odd_imag = section[1, :, :, :128], section[1, :, :, 128:]
        odd_real, odd_imag = turned(odd_real, odd_imag, turns[0], turns[1])
        halves = (
            turned(even_real + odd_real, even_imag + odd_imag, turns[2], turns[3]),
            turned(even_real - odd_real, even_imag - odd_imag, turns[4], turns[5]),
        )
        both = jnp.concatenate(
            [
                jnp.concatenate([real.reshape(128, 128), imag.reshape(128, 128)], axis=1)
                for real, imag in halves
            ],
            axis=0,
        )
        high = both.astype(jnp.bfloat16)
        low = (both - high.astype(jnp.float32)).astype(jnp.bfloat16)
        result = dot(high, last_hi[...]) + dot(low, last_hi[...]) + dot(high, last_lo[...])
        for half in range(2):
            for part in range(2):
                out[group, part, :, half * 16 : half * 16 + 16, :] = result[
                    half * 128 : (half + 1) * 128, part * 128 : (part + 1) * 128
                ].reshape(8, 16, 128)
        if group > 0:
            store(group - 1).start()
    store(groups - 1).start()
    for group in range(groups):
        store(group).wait()


def transform(received):
    (first_hi, first_lo), turns, (last_hi, last_lo) = transform_tables()
    return pl.pallas_call(
        transform_kernel,
        out_shape=jax.ShapeDtypeStruct((2, 8, 8, 1, FFT_LO, FFT_HI), jnp.float32),
        in_specs=[pl.BlockSpec(memory_space=pltpu.VMEM)] * 6,
        out_specs=pl.BlockSpec(memory_space=pltpu.HBM),
        scratch_shapes=[
            pltpu.VMEM((8, 2, 8, FFT_LO, FFT_HI), jnp.float32),
            pltpu.SemaphoreType.DMA,
        ],
        compiler_params=pltpu.CompilerParams(vmem_limit_bytes=32 * 1024 * 1024),
    )(received, first_hi, first_lo, turns, last_hi, last_lo)


def shards(strengths, sample_cell, sample_frac):
    return transform(spread(strengths, sample_cell, sample_frac))


def solution(mesh):
    placed = (P(None, "freq", None, "tm"), P("tm"), P("tm"))
    return jax.shard_map(
        shards,
        mesh=mesh,
        in_specs=placed,
        out_specs=P(None, None, "tm", "freq", None, None),
        check_vma=False,
    )
```

```python
import math

import jax
import jax.numpy as jnp
import numpy as np
from jax import lax
from jax.experimental import pallas as pl
from jax.experimental.pallas import tpu as pltpu
from jax.sharding import PartitionSpec as P

TAPS = 8
GRID_DEV = 1024
FFT_LO = 32
FFT_HI = 128
FFTLEN = 4096
MESH = pl.DeviceIdType.MESH

sharpness = 0.3

BLOCKS = 32
CHUNKS = 4
CHUNK = GRID_DEV // CHUNKS
TILE = 16
HALVES = 2
PAIRS = 4
MESSAGE = (8, CHUNK)


def plane(step, own):
    shift = ((step + 1) >> 1) * (2 * (step & 1) - 1)
    return (own + shift + 8) & 7


def transform_pair(data, first_hi, first_lo, turns, last_hi, last_lo):
    def dot(a, b):
        return jnp.dot(a, b, preferred_element_type=jnp.float32)

    def turned(real, imag, cos, sin):
        return real * cos + imag * sin, imag * cos - real * sin

    section = dot(first_hi[...], data) + dot(first_lo[...], data)
    section = section.reshape(2, 8, 16, 256)
    even_real, odd_real = section[0, :, :, :128], section[0, :, :, 128:]
    even_imag, odd_imag = section[1, :, :, :128], section[1, :, :, 128:]
    odd_real, odd_imag = turned(odd_real, odd_imag, turns[0], turns[1])
    halves = (
        turned(even_real + odd_real, even_imag + odd_imag, turns[2], turns[3]),
        turned(even_real - odd_real, even_imag - odd_imag, turns[4], turns[5]),
    )
    both = jnp.concatenate(
        [
            jnp.concatenate([real.reshape(128, 128), imag.reshape(128, 128)], axis=1)
            for real, imag in halves
        ],
        axis=0,
    )
    high = both.astype(jnp.bfloat16)
    return dot(high, last_hi[...]) + dot(high, last_lo[...])


def store_pair(out, pair, result):
    for half in range(2):
        for part in range(2):
            out[pair, part, :, :, half * 16 : half * 16 + 16, :] = result[
                half * 128 : (half + 1) * 128, part * 128 : (part + 1) * 128
            ].reshape(2, 4, 16, 128)


def spread_kernel(
    strength_hbm,
    cell_hbm,
    frac_hbm,
    first_hi_hbm,
    first_lo_hbm,
    turns_hbm,
    last_hi_hbm,
    last_lo_hbm,
    second,
    spectra,
    cell_ref,
    frac_ref,
    strength,
    window,
    outgoing,
    first,
    partial,
    halo,
    halo_in,
    first_hi,
    first_lo,
    turns,
    last_hi,
    last_lo,
    load_sem,
    table_sem,
    send_sem,
    recv_sem,
    halo_send_sem,
    halo_recv_sem,
):
    block = lax.axis_index("tm")
    group = lax.axis_index("freq")
    frame = block // 4
    right, left = (block + 1) % BLOCKS, (block + BLOCKS - 1) % BLOCKS

    loads = [
        pltpu.make_async_copy(cell_hbm, cell_ref, load_sem.at[0]),
        pltpu.make_async_copy(frac_hbm, frac_ref, load_sem.at[1]),
        pltpu.make_async_copy(strength_hbm, strength, load_sem.at[2]),
    ]
    for load in loads:
        load.start()

    barrier = pltpu.get_barrier_semaphore()

    def greet(i, carry):
        pl.semaphore_signal(
            barrier, inc=1, device_id=(4 * group + (i >> 3), i & 7), device_id_type=MESH
        )
        return carry

    lax.fori_loop(0, BLOCKS, greet, 0)
    for beside in (left, right):
        pl.semaphore_signal(barrier, inc=1, device_id=(beside, group), device_id_type=MESH)

    tables = [
        pltpu.make_async_copy(src, dst, table_sem.at[i])
        for i, (src, dst) in enumerate(
            (
                (first_hi_hbm, first_hi),
                (first_lo_hbm, first_lo),
                (turns_hbm, turns),
                (last_hi_hbm, last_hi),
                (last_lo_hbm, last_lo),
            )
        )
    ]
    for table in tables:
        table.start()

    loads[0].wait()
    loads[1].wait()
    samples = cell_ref.shape[1]
    start = jnp.broadcast_to(
        cell_ref[...] - block * GRID_DEV + (TILE - (TAPS // 2 - 1)), (TILE, samples)
    )
    row = lax.broadcasted_iota(jnp.int32, (TILE, samples), 0)
    phase = start & (TILE - 1)
    tap = (row - phase) & (TILE - 1)
    shifted = tap.astype(jnp.float32) - float(TAPS // 2 - 1) - frac_ref[...]
    values = jnp.exp(-sharpness * (shifted * shifted))
    values = jnp.where(tap < TAPS, values, 0.0).astype(jnp.bfloat16)
    tile_of = (lax.shift_right_logical(start, 4) + jnp.where(row < phase, 1, 0)).astype(
        jnp.float32
    )
    edge = jnp.where(row < TILE // 2, float(GRID_DEV // TILE + 1), 0.0)
    nothing = jnp.zeros_like(values)
    edge_window = jnp.where(tile_of == edge, values.astype(jnp.float32), 0.0).astype(jnp.bfloat16)
    tile_of = tile_of.astype(jnp.bfloat16)

    def build(chunk):
        for i in range(CHUNK // TILE):
            q = chunk * (CHUNK // TILE) + i
            window[q * TILE : (q + 1) * TILE, :] = jnp.where(
                tile_of == jnp.bfloat16(q + 1), values, nothing
            )

    across = (((1,), (1,)), ((), ()))

    def rows():
        return strength[...].reshape(2 * strength.shape[2], samples)

    def gather(chunk):
        return lax.dot_general(
            rows(),
            window[chunk * CHUNK : (chunk + 1) * CHUNK, :],
            across,
            preferred_element_type=jnp.float32,
        )

    def round_out(chunk, total):
        channels = total.shape[0] // 2
        real = total[:channels].reshape(BLOCKS, 8, CHUNK)
        imag = total[channels:].reshape(BLOCKS, 8, CHUNK)
        upper = lax.broadcasted_iota(jnp.int32, real.shape, 1) < 4
        outgoing[0, :, chunk] = jnp.where(upper, real, pltpu.roll(imag, 4, 1)).astype(jnp.bfloat16)
        outgoing[1, :, chunk] = jnp.where(upper, pltpu.roll(real, 4, 1), imag).astype(jnp.bfloat16)

    own_plane = (block >> 1) & 7
    offsets = [
        (((block >> 4) + (inner >> 1)) & 1) * 16 + ((block + inner) & 1) for inner in range(4)
    ]

    def send(half, begin, count):
        landing = (first, second)[half]
        dst = landing.at[group // 2, block % 4, group % 2, pl.ds(begin, count)]

        def one(step, carry):
            position = plane(step, own_plane)
            for inner in range(4):
                target = offsets[inner] + 2 * position
                src = outgoing.at[half, target, pl.ds(begin, count)]
                remote = pltpu.make_async_remote_copy(
                    src_ref=src,
                    dst_ref=dst,
                    send_sem=send_sem,
                    recv_sem=recv_sem.at[half],
                    device_id=(target, frame),
                    device_id_type=MESH,
                )
                if inner:
                    remote.start()
                    continue
                own = jnp.logical_and(position == own_plane, frame == group)

                @pl.when(jnp.logical_not(own))
                def _():
                    remote.start()

                @pl.when(own)
                def _():
                    pltpu.make_async_copy(src, dst, recv_sem.at[half]).start()

            return carry

        lax.fori_loop(0, 8, one, 0)

    build(1)
    loads[2].wait()
    round_out(1, gather(1))
    build(2)
    round_out(2, gather(2))
    halo[...] = lax.dot_general(edge_window, rows(), across, preferred_element_type=jnp.float32)

    pl.semaphore_wait(barrier, 34)
    to_right = pltpu.make_async_remote_copy(
        src_ref=halo.at[0:8],
        dst_ref=halo_in.at[0:8],
        send_sem=halo_send_sem,
        recv_sem=halo_recv_sem,
        device_id=(right, group),
        device_id_type=MESH,
    )
    to_left = pltpu.make_async_remote_copy(
        src_ref=halo.at[8:16],
        dst_ref=halo_in.at[120:128],
        send_sem=halo_send_sem,
        recv_sem=halo_recv_sem,
        device_id=(left, group),
        device_id_type=MESH,
    )
    to_right.start()
    to_left.start()
    send(0, 1, 2)

    build(0)
    partial[0] = gather(0)
    build(3)
    partial[1] = gather(3)
    halo_in[8:120, :] = jnp.zeros((112, halo_in.shape[1]), jnp.float32)

    pltpu.make_async_copy(halo, halo_in.at[0:16], halo_recv_sem).wait()
    beyond = halo_in[...].T
    lane = lax.broadcasted_iota(jnp.int32, beyond.shape, 1)
    none = jnp.zeros((beyond.shape[0], CHUNK - 128), jnp.float32)
    round_out(
        0, partial[0] + jnp.concatenate([jnp.where(lane < 8, beyond, 0.0), none], axis=1)
    )
    send(0, 0, 1)
    round_out(
        3, partial[1] + jnp.concatenate([none, jnp.where(lane >= 120, beyond, 0.0)], axis=1)
    )
    send(0, 3, 1)
    send(1, 0, 4)

    for table in tables:
        table.wait()
    pltpu.make_async_copy(outgoing.at[0], first, recv_sem.at[0]).wait()

    def one_pair(pair, carry):
        data = first[pair].reshape(256, 256)
        store_pair(
            spectra, pair, transform_pair(data, first_hi, first_lo, turns, last_hi, last_lo)
        )
        return carry

    lax.fori_loop(0, PAIRS, one_pair, 0)

    pltpu.make_async_copy(halo, halo_in.at[0:16], halo_send_sem).wait()

    @pl.when(frame == group)
    def _():
        pltpu.make_async_copy(outgoing.at[:, 0:31], outgoing.at[:, 0:31], send_sem).wait()

    @pl.when(frame != group)
    def _():
        pltpu.make_async_copy(outgoing, outgoing, send_sem).wait()

    pltpu.make_async_copy(outgoing.at[1], second, recv_sem.at[1]).wait()


def spread(strengths, sample_cell, sample_frac, tables):
    channels, samples = strengths.shape[2], strengths.shape[3]
    rows = 2 * channels
    half_shape = (PAIRS, 4, 2, CHUNKS, *MESSAGE)
    inputs = (
        strengths,
        sample_cell.reshape(1, samples),
        sample_frac.reshape(1, samples),
        *tables,
    )
    return pl.pallas_call(
        spread_kernel,
        out_shape=(
            jax.ShapeDtypeStruct(half_shape, jnp.bfloat16),
            jax.ShapeDtypeStruct((PAIRS, 2, 2, 4, FFT_LO, FFT_HI), jnp.float32),
        ),
        in_specs=[pl.BlockSpec(memory_space=pltpu.HBM)] * len(inputs),
        out_specs=(pl.BlockSpec(memory_space=pltpu.VMEM),) * 2,
        scratch_shapes=[
            pltpu.VMEM((1, samples), jnp.int32),
            pltpu.VMEM((1, samples), jnp.float32),
            pltpu.VMEM(strengths.shape, jnp.bfloat16),
            pltpu.VMEM((GRID_DEV, samples), jnp.bfloat16),
            pltpu.VMEM((HALVES, BLOCKS, CHUNKS, *MESSAGE), jnp.bfloat16),
            pltpu.VMEM(half_shape, jnp.bfloat16),
            pltpu.VMEM((2, rows, CHUNK), jnp.float32),
            pltpu.VMEM((16, rows), jnp.float32),
            pltpu.VMEM((128, rows), jnp.float32),
            *(pltpu.VMEM(table.shape, table.dtype) for table in tables),
            pltpu.SemaphoreType.DMA((3,)),
            pltpu.SemaphoreType.DMA((5,)),
            pltpu.SemaphoreType.DMA,
            pltpu.SemaphoreType.DMA((2,)),
            pltpu.SemaphoreType.DMA,
            pltpu.SemaphoreType.DMA,
        ],
        compiler_params=pltpu.CompilerParams(
            collective_id=0, has_side_effects=True, vmem_limit_bytes=48 * 1024 * 1024
        ),
    )(*(pltpu.with_memory_space_constraint(x, pltpu.HBM) for x in inputs))


def split_bf16(table):
    high = table.astype(jnp.bfloat16)
    low = (table - high.astype(np.float64)).astype(jnp.bfloat16)
    return high, low


def transform_tables():
    digit = np.arange(16)
    angle = 2.0 * math.pi * (digit[:, None] * digit[None, :] % 16) / 16
    cos, sin = np.cos(angle), np.sin(angle)
    group, channel = np.eye(2), np.eye(4)

    def entry(part):
        return np.einsum("atm,gh,cd->gcathmd", part.reshape(16, 4, 4), group, channel)

    first = np.zeros((2, 2, 4, 16, 4, 2, 4, 2, 4))
    first[0, ..., 0, :] = entry(cos)
    first[0, ..., 1, :] = entry(sin)
    first[1, ..., 0, :] = entry(-sin)
    first[1, ..., 1, :] = entry(cos)
    first = first.reshape(256, 256)

    n = np.arange(FFT_HI)
    half_turn = 2.0 * math.pi * digit[:, None] / FFT_LO * np.ones((1, FFT_HI))
    turn = 2.0 * math.pi * np.arange(FFT_LO)[:, None] * n[None, :] / FFTLEN
    turns = np.stack(
        [
            np.cos(half_turn),
            np.sin(half_turn),
            np.cos(turn[:16]),
            np.sin(turn[:16]),
            np.cos(turn[16:]),
            np.sin(turn[16:]),
        ]
    ).astype(np.float32)

    angle = 2.0 * math.pi * (n[:, None] * n[None, :] % FFT_HI) / FFT_HI
    cos, sin = np.cos(angle), np.sin(angle)
    last = np.block([[cos, -sin], [sin, cos]]) / math.sqrt(FFTLEN)
    return (*split_bf16(first), turns, *split_bf16(last))


def finish_kernel(
    data_ref, done, first_hi, first_lo, turns, last_hi, last_lo, out_hbm, out, done_sem, sem
):
    def place(src, half, pair, semaphore):
        return pltpu.make_async_copy(
            src.at[pair],
            out_hbm.at[:, pl.ds(2 * pair, 2), pl.ds(4 * half, 4), 0],
            semaphore,
        )

    for pair in range(PAIRS):
        place(done, 0, pair, done_sem).start()
    for pair in range(PAIRS):
        data = data_ref[pair].reshape(256, 256)
        store_pair(
            out, pair, transform_pair(data, first_hi, first_lo, turns, last_hi, last_lo)
        )
    for pair in range(PAIRS):
        place(out, 1, pair, sem).start()
    for pair in range(PAIRS):
        place(done, 0, pair, done_sem).wait()
    for pair in range(PAIRS):
        place(out, 1, pair, sem).wait()


def finish(second, spectra, tables):
    return pl.pallas_call(
        finish_kernel,
        out_shape=jax.ShapeDtypeStruct((2, 8, 8, 1, FFT_LO, FFT_HI), jnp.float32),
        in_specs=[pl.BlockSpec(memory_space=pltpu.VMEM)] * 7,
        out_specs=pl.BlockSpec(memory_space=pltpu.HBM),
        scratch_shapes=[
            pltpu.VMEM((PAIRS, 2, 2, 4, FFT_LO, FFT_HI), jnp.float32),
            pltpu.SemaphoreType.DMA,
            pltpu.SemaphoreType.DMA,
        ],
        compiler_params=pltpu.CompilerParams(vmem_limit_bytes=32 * 1024 * 1024),
    )(second, spectra, *tables)


def shards(strengths, sample_cell, sample_frac):
    tables = tuple(jnp.asarray(table) for table in transform_tables())
    second, spectra = spread(strengths, sample_cell, sample_frac, tables)
    return finish(second, spectra, tables)


def solution(mesh):
    placed = (P(None, "freq", None, "tm"), P("tm"), P("tm"))
    return jax.shard_map(
        shards,
        mesh=mesh,
        in_specs=placed,
        out_specs=P(None, None, "tm", "freq", None, None),
        check_vma=False,
    )
```

```python
import math

import jax
import jax.numpy as jnp
import numpy as np
from jax import lax
from jax.experimental import pallas as pl
from jax.experimental.pallas import tpu as pltpu
from jax.sharding import PartitionSpec as P

TAPS = 8
GRID_DEV = 1024
FFT_LO = 32
FFT_HI = 128
FFTLEN = 4096
MESH = pl.DeviceIdType.MESH

sharpness = 0.3

BLOCKS = 32
CHUNKS = 4
CHUNK = GRID_DEV // CHUNKS
TILE = 16
HALVES = 2
PIECES = 4
PIECE = 512
PAIRS = 4
MESSAGE = (8, CHUNK)


def plane(step, own):
    shift = ((step + 1) >> 1) * (2 * (step & 1) - 1)
    return (own + shift + 8) & 7


def transform_pair(data, first_hi, first_lo, turns, last_hi, last_lo):
    def dot(a, b):
        return jnp.dot(a, b, preferred_element_type=jnp.float32)

    def turned(real, imag, cos, sin):
        return real * cos + imag * sin, imag * cos - real * sin

    section = dot(first_hi[...], data) + dot(first_lo[...], data)
    section = section.reshape(2, 8, 16, 256)
    even_real, odd_real = section[0, :, :, :128], section[0, :, :, 128:]
    even_imag, odd_imag = section[1, :, :, :128], section[1, :, :, 128:]
    odd_real, odd_imag = turned(odd_real, odd_imag, turns[0], turns[1])
    halves = (
        turned(even_real + odd_real, even_imag + odd_imag, turns[2], turns[3]),
        turned(even_real - odd_real, even_imag - odd_imag, turns[4], turns[5]),
    )
    both = jnp.concatenate(
        [
            jnp.concatenate([real.reshape(128, 128), imag.reshape(128, 128)], axis=1)
            for real, imag in halves
        ],
        axis=0,
    )
    high = both.astype(jnp.bfloat16)
    return dot(high, last_hi[...]) + dot(high, last_lo[...])


def store_pair(out, pair, result):
    for half in range(2):
        for part in range(2):
            out[pair, part, :, :, half * 16 : half * 16 + 16, :] = result[
                half * 128 : (half + 1) * 128, part * 128 : (part + 1) * 128
            ].reshape(2, 4, 16, 128)


def spread_kernel(
    strength_hbm,
    cell_hbm,
    frac_hbm,
    first_hi_hbm,
    first_lo_hbm,
    turns_hbm,
    last_hi_hbm,
    last_lo_hbm,
    second,
    spectra,
    first_hi,
    first_lo,
    turns,
    last_hi,
    last_lo,
    cell_ref,
    frac_ref,
    strength,
    window,
    outgoing,
    first,
    partial,
    halo,
    halo_in,
    load_sem,
    table_sem,
    send_sem,
    recv_sem,
    halo_send_sem,
    halo_recv_sem,
):
    block = lax.axis_index("tm")
    group = lax.axis_index("freq")
    frame = block // 4
    right, left = (block + 1) % BLOCKS, (block + BLOCKS - 1) % BLOCKS

    loads = [
        pltpu.make_async_copy(cell_hbm, cell_ref, load_sem.at[0]),
        pltpu.make_async_copy(frac_hbm, frac_ref, load_sem.at[1]),
        *(
            pltpu.make_async_copy(
                strength_hbm.at[:, :, :, pl.ds(piece * PIECE, PIECE)],
                strength.at[:, :, :, pl.ds(piece * PIECE, PIECE)],
                load_sem.at[2 + piece],
            )
            for piece in range(PIECES)
        ),
    ]
    for load in loads:
        load.start()

    barrier = pltpu.get_barrier_semaphore()

    def greet(i, carry):
        pl.semaphore_signal(
            barrier, inc=1, device_id=(4 * group + (i >> 3), i & 7), device_id_type=MESH
        )
        return carry

    lax.fori_loop(0, BLOCKS, greet, 0)
    for beside in (left, right):
        pl.semaphore_signal(barrier, inc=1, device_id=(beside, group), device_id_type=MESH)

    tables = [
        pltpu.make_async_copy(src, dst, table_sem.at[i])
        for i, (src, dst) in enumerate(
            (
                (first_hi_hbm, first_hi),
                (first_lo_hbm, first_lo),
                (turns_hbm, turns),
                (last_hi_hbm, last_hi),
                (last_lo_hbm, last_lo),
            )
        )
    ]
    loads[0].wait()
    loads[1].wait()
    samples = cell_ref.shape[1]
    start = jnp.broadcast_to(
        cell_ref[...] - block * GRID_DEV + (TILE - (TAPS // 2 - 1)), (TILE, samples)
    )
    row = lax.broadcasted_iota(jnp.int32, (TILE, samples), 0)
    phase = start & (TILE - 1)
    tap = (row - phase) & (TILE - 1)
    shifted = tap.astype(jnp.float32) - float(TAPS // 2 - 1) - frac_ref[...]
    values = jnp.exp(-sharpness * (shifted * shifted))
    values = jnp.where(tap < TAPS, values, 0.0).astype(jnp.bfloat16)
    tile_of = (lax.shift_right_logical(start, 4) + jnp.where(row < phase, 1, 0)).astype(
        jnp.float32
    )
    edge = jnp.where(row < TILE // 2, float(GRID_DEV // TILE + 1), 0.0)
    nothing = jnp.zeros_like(values)
    edge_window = jnp.where(tile_of == edge, values.astype(jnp.float32), 0.0).astype(jnp.bfloat16)
    tile_of = tile_of.astype(jnp.bfloat16)

    def build(chunk):
        for i in range(CHUNK // TILE):
            q = chunk * (CHUNK // TILE) + i
            window[q * TILE : (q + 1) * TILE, :] = jnp.where(
                tile_of == jnp.bfloat16(q + 1), values, nothing
            )

    across = (((1,), (1,)), ((), ()))

    def rows():
        return strength[...].reshape(2 * strength.shape[2], samples)

    def gather(chunk):
        return lax.dot_general(
            rows(),
            window[chunk * CHUNK : (chunk + 1) * CHUNK, :],
            across,
            preferred_element_type=jnp.float32,
        )

    def round_out(chunk, total):
        channels = total.shape[0] // 2
        real = total[:channels].reshape(BLOCKS, 8, CHUNK)
        imag = total[channels:].reshape(BLOCKS, 8, CHUNK)
        upper = lax.broadcasted_iota(jnp.int32, real.shape, 1) < 4
        outgoing[0, :, chunk] = jnp.where(upper, real, pltpu.roll(imag, 4, 1)).astype(jnp.bfloat16)
        outgoing[1, :, chunk] = jnp.where(upper, pltpu.roll(real, 4, 1), imag).astype(jnp.bfloat16)

    own_plane = (block >> 1) & 7
    offsets = [
        (((block >> 4) + (inner >> 1)) & 1) * 16 + ((block + inner) & 1) for inner in range(4)
    ]

    def send(half, begin, count):
        landing = (first, second)[half]
        dst = landing.at[group // 2, block % 4, group % 2, pl.ds(begin, count)]

        def one(step, carry):
            position = plane(step, own_plane)
            for inner in range(4):
                target = offsets[inner] + 2 * position
                src = outgoing.at[half, target, pl.ds(begin, count)]
                remote = pltpu.make_async_remote_copy(
                    src_ref=src,
                    dst_ref=dst,
                    send_sem=send_sem,
                    recv_sem=recv_sem.at[half],
                    device_id=(target, frame),
                    device_id_type=MESH,
                )
                if inner:
                    remote.start()
                    continue
                own = jnp.logical_and(position == own_plane, frame == group)

                @pl.when(jnp.logical_not(own))
                def _():
                    remote.start()

                @pl.when(own)
                def _():
                    pltpu.make_async_copy(src, dst, recv_sem.at[half]).start()

            return carry

        lax.fori_loop(0, 8, one, 0)

    build(1)
    total = None
    for piece in range(PIECES):
        loads[2 + piece].wait()
        span = slice(piece * PIECE, (piece + 1) * PIECE)
        part = lax.dot_general(
            strength[:, :, :, span].reshape(2 * strength.shape[2], PIECE),
            window[CHUNK : 2 * CHUNK, span],
            across,
            preferred_element_type=jnp.float32,
        )
        total = part if total is None else total + part
    round_out(1, total)
    pl.semaphore_wait(barrier, 34)
    send(0, 1, 1)
    for table in tables:
        table.start()
    halo[...] = lax.dot_general(edge_window, rows(), across, preferred_element_type=jnp.float32)
    to_right = pltpu.make_async_remote_copy(
        src_ref=halo.at[0:8],
        dst_ref=halo_in.at[0:8],
        send_sem=halo_send_sem,
        recv_sem=halo_recv_sem,
        device_id=(right, group),
        device_id_type=MESH,
    )
    to_left = pltpu.make_async_remote_copy(
        src_ref=halo.at[8:16],
        dst_ref=halo_in.at[120:128],
        send_sem=halo_send_sem,
        recv_sem=halo_recv_sem,
        device_id=(left, group),
        device_id_type=MESH,
    )
    to_right.start()
    to_left.start()
    build(2)
    round_out(2, gather(2))
    send(0, 2, 1)
    build(0)
    partial[0] = gather(0)
    build(3)
    partial[1] = gather(3)
    halo_in[8:120, :] = jnp.zeros((112, halo_in.shape[1]), jnp.float32)

    pltpu.make_async_copy(halo, halo_in.at[0:16], halo_recv_sem).wait()
    beyond = halo_in[...].T
    lane = lax.broadcasted_iota(jnp.int32, beyond.shape, 1)
    none = jnp.zeros((beyond.shape[0], CHUNK - 128), jnp.float32)
    round_out(
        0, partial[0] + jnp.concatenate([jnp.where(lane < 8, beyond, 0.0), none], axis=1)
    )
    send(0, 0, 1)
    round_out(
        3, partial[1] + jnp.concatenate([none, jnp.where(lane >= 120, beyond, 0.0)], axis=1)
    )
    send(0, 3, 1)
    send(1, 0, 4)

    for table in tables:
        table.wait()
    pltpu.make_async_copy(outgoing.at[0], first, recv_sem.at[0]).wait()

    def one_pair(pair, carry):
        data = first[pair].reshape(256, 256)
        store_pair(
            spectra, pair, transform_pair(data, first_hi, first_lo, turns, last_hi, last_lo)
        )
        return carry

    lax.fori_loop(0, PAIRS, one_pair, 0)

    pltpu.make_async_copy(halo, halo_in.at[0:16], halo_send_sem).wait()

    @pl.when(frame == group)
    def _():
        pltpu.make_async_copy(outgoing.at[:, 0:31], outgoing.at[:, 0:31], send_sem).wait()

    @pl.when(frame != group)
    def _():
        pltpu.make_async_copy(outgoing, outgoing, send_sem).wait()

    pltpu.make_async_copy(outgoing.at[1], second, recv_sem.at[1]).wait()


def spread(strengths, sample_cell, sample_frac, tables):
    channels, samples = strengths.shape[2], strengths.shape[3]
    rows = 2 * channels
    half_shape = (PAIRS, 4, 2, CHUNKS, *MESSAGE)
    inputs = (
        strengths,
        sample_cell.reshape(1, samples),
        sample_frac.reshape(1, samples),
        *tables,
    )
    return pl.pallas_call(
        spread_kernel,
        out_shape=(
            jax.ShapeDtypeStruct(half_shape, jnp.bfloat16),
            jax.ShapeDtypeStruct((PAIRS, 2, 2, 4, FFT_LO, FFT_HI), jnp.float32),
            *(jax.ShapeDtypeStruct(table.shape, table.dtype) for table in tables),
        ),
        in_specs=[pl.BlockSpec(memory_space=pltpu.HBM)] * len(inputs),
        out_specs=(pl.BlockSpec(memory_space=pltpu.VMEM),) * (2 + len(tables)),
        scratch_shapes=[
            pltpu.VMEM((1, samples), jnp.int32),
            pltpu.VMEM((1, samples), jnp.float32),
            pltpu.VMEM(strengths.shape, jnp.bfloat16),
            pltpu.VMEM((GRID_DEV, samples), jnp.bfloat16),
            pltpu.VMEM((HALVES, BLOCKS, CHUNKS, *MESSAGE), jnp.bfloat16),
            pltpu.VMEM(half_shape, jnp.bfloat16),
            pltpu.VMEM((2, rows, CHUNK), jnp.float32),
            pltpu.VMEM((16, rows), jnp.float32),
            pltpu.VMEM((128, rows), jnp.float32),
            pltpu.SemaphoreType.DMA((2 + PIECES,)),
            pltpu.SemaphoreType.DMA((5,)),
            pltpu.SemaphoreType.DMA,
            pltpu.SemaphoreType.DMA((2,)),
            pltpu.SemaphoreType.DMA,
            pltpu.SemaphoreType.DMA,
        ],
        compiler_params=pltpu.CompilerParams(
            collective_id=0, has_side_effects=True, vmem_limit_bytes=48 * 1024 * 1024
        ),
    )(*(pltpu.with_memory_space_constraint(x, pltpu.HBM) for x in inputs))


def split_bf16(table):
    high = table.astype(jnp.bfloat16)
    low = (table - high.astype(np.float64)).astype(jnp.bfloat16)
    return high, low


def transform_tables():
    digit = np.arange(16)
    angle = 2.0 * math.pi * (digit[:, None] * digit[None, :] % 16) / 16
    cos, sin = np.cos(angle), np.sin(angle)
    group, channel = np.eye(2), np.eye(4)

    def entry(part):
        return np.einsum("atm,gh,cd->gcathmd", part.reshape(16, 4, 4), group, channel)

    first = np.zeros((2, 2, 4, 16, 4, 2, 4, 2, 4))
    first[0, ..., 0, :] = entry(cos)
    first[0, ..., 1, :] = entry(sin)
    first[1, ..., 0, :] = entry(-sin)
    first[1, ..., 1, :] = entry(cos)
    first = first.reshape(256, 256)

    n = np.arange(FFT_HI)
    half_turn = 2.0 * math.pi * digit[:, None] / FFT_LO * np.ones((1, FFT_HI))
    turn = 2.0 * math.pi * np.arange(FFT_LO)[:, None] * n[None, :] / FFTLEN
    turns = np.stack(
        [
            np.cos(half_turn),
            np.sin(half_turn),
            np.cos(turn[:16]),
            np.sin(turn[:16]),
            np.cos(turn[16:]),
            np.sin(turn[16:]),
        ]
    ).astype(np.float32)

    angle = 2.0 * math.pi * (n[:, None] * n[None, :] % FFT_HI) / FFT_HI
    cos, sin = np.cos(angle), np.sin(angle)
    last = np.block([[cos, -sin], [sin, cos]]) / math.sqrt(FFTLEN)
    return (*split_bf16(first), turns, *split_bf16(last))


def finish_kernel(
    data_ref, done, first_hi, first_lo, turns, last_hi, last_lo, out_hbm, out, done_sem, sem
):
    def place(src, half, pair, semaphore):
        return pltpu.make_async_copy(
            src.at[pair],
            out_hbm.at[:, pl.ds(2 * pair, 2), pl.ds(4 * half, 4), 0],
            semaphore,
        )

    for pair in range(PAIRS):
        place(done, 0, pair, done_sem).start()
    for pair in range(PAIRS):
        data = data_ref[pair].reshape(256, 256)
        store_pair(
            out, pair, transform_pair(data, first_hi, first_lo, turns, last_hi, last_lo)
        )
    for pair in range(PAIRS):
        place(out, 1, pair, sem).start()
    for pair in range(PAIRS):
        place(done, 0, pair, done_sem).wait()
    for pair in range(PAIRS):
        place(out, 1, pair, sem).wait()


def finish(second, spectra, tables):
    return pl.pallas_call(
        finish_kernel,
        out_shape=jax.ShapeDtypeStruct((2, 8, 8, 1, FFT_LO, FFT_HI), jnp.float32),
        in_specs=[pl.BlockSpec(memory_space=pltpu.VMEM)] * 7,
        out_specs=pl.BlockSpec(memory_space=pltpu.HBM),
        scratch_shapes=[
            pltpu.VMEM((PAIRS, 2, 2, 4, FFT_LO, FFT_HI), jnp.float32),
            pltpu.SemaphoreType.DMA,
            pltpu.SemaphoreType.DMA,
        ],
        compiler_params=pltpu.CompilerParams(vmem_limit_bytes=32 * 1024 * 1024),
    )(second, spectra, *tables)


def shards(strengths, sample_cell, sample_frac):
    tables = tuple(jnp.asarray(table) for table in transform_tables())
    second, spectra, *tables = spread(strengths, sample_cell, sample_frac, tables)
    return finish(second, spectra, tables)


def solution(mesh):
    placed = (P(None, "freq", None, "tm"), P("tm"), P("tm"))
    return jax.shard_map(
        shards,
        mesh=mesh,
        in_specs=placed,
        out_specs=P(None, None, "tm", "freq", None, None),
        check_vma=False,
    )
```

```python
import math

import jax
import jax.numpy as jnp
import numpy as np
from jax import lax
from jax.experimental import pallas as pl
from jax.experimental.pallas import tpu as pltpu
from jax.sharding import PartitionSpec as P

TAPS = 8
GRID_DEV = 1024
FFT_LO = 32
FFT_HI = 128
FFTLEN = 4096
MESH = pl.DeviceIdType.MESH

sharpness = 0.3

BLOCKS = 32
CHUNKS = 4
CHUNK = GRID_DEV // CHUNKS
TILE = 16
HALVES = 2
PIECES = 4
PIECE = 512
PAIRS = 4
MESSAGE = (8, CHUNK)


def plane(step, own, far):
    count = (1 - far) * step + far * (7 - step)
    shift = ((count + 1) >> 1) * (2 * (count & 1) - 1)
    return (own + shift + 8) & 7


def transform_pair(data, first_hi, first_lo, turns, last_hi, last_lo):
    def dot(a, b):
        return jnp.dot(a, b, preferred_element_type=jnp.float32)

    def turned(real, imag, cos, sin):
        return real * cos + imag * sin, imag * cos - real * sin

    section = dot(first_hi[...], data) + dot(first_lo[...], data)
    section = section.reshape(2, 8, 16, 256)
    even_real, odd_real = section[0, :, :, :128], section[0, :, :, 128:]
    even_imag, odd_imag = section[1, :, :, :128], section[1, :, :, 128:]
    odd_real, odd_imag = turned(odd_real, odd_imag, turns[0], turns[1])
    halves = (
        turned(even_real + odd_real, even_imag + odd_imag, turns[2], turns[3]),
        turned(even_real - odd_real, even_imag - odd_imag, turns[4], turns[5]),
    )
    both = jnp.concatenate(
        [
            jnp.concatenate([real.reshape(128, 128), imag.reshape(128, 128)], axis=1)
            for real, imag in halves
        ],
        axis=0,
    )
    high = both.astype(jnp.bfloat16)
    return dot(high, last_hi[...]) + dot(high, last_lo[...])


def store_pair(out, pair, result):
    for half in range(2):
        for part in range(2):
            out[pair, part, :, :, half * 16 : half * 16 + 16, :] = result[
                half * 128 : (half + 1) * 128, part * 128 : (part + 1) * 128
            ].reshape(2, 4, 16, 128)


def spread_kernel(
    strength_hbm,
    cell_hbm,
    frac_hbm,
    first_hi_hbm,
    first_lo_hbm,
    turns_hbm,
    last_hi_hbm,
    last_lo_hbm,
    second,
    spectra,
    first_hi,
    first_lo,
    turns,
    last_hi,
    last_lo,
    cell_ref,
    frac_ref,
    strength,
    window,
    outgoing,
    first,
    partial,
    halo,
    halo_in,
    load_sem,
    table_sem,
    send_sem,
    recv_sem,
    halo_send_sem,
    halo_recv_sem,
):
    block = lax.axis_index("tm")
    group = lax.axis_index("freq")
    frame = block // 4
    right, left = (block + 1) % BLOCKS, (block + BLOCKS - 1) % BLOCKS

    loads = [
        pltpu.make_async_copy(cell_hbm, cell_ref, load_sem.at[0]),
        pltpu.make_async_copy(frac_hbm, frac_ref, load_sem.at[1]),
        *(
            pltpu.make_async_copy(
                strength_hbm.at[:, :, :, pl.ds(piece * PIECE, PIECE)],
                strength.at[:, :, :, pl.ds(piece * PIECE, PIECE)],
                load_sem.at[2 + piece],
            )
            for piece in range(PIECES)
        ),
    ]
    for load in loads:
        load.start()

    barrier = pltpu.get_barrier_semaphore()

    def greet(i, carry):
        pl.semaphore_signal(
            barrier, inc=1, device_id=(4 * group + (i >> 3), i & 7), device_id_type=MESH
        )
        return carry

    lax.fori_loop(0, BLOCKS, greet, 0)
    for beside in (left, right):
        pl.semaphore_signal(barrier, inc=1, device_id=(beside, group), device_id_type=MESH)

    tables = [
        pltpu.make_async_copy(src, dst, table_sem.at[i])
        for i, (src, dst) in enumerate(
            (
                (first_hi_hbm, first_hi),
                (first_lo_hbm, first_lo),
                (turns_hbm, turns),
                (last_hi_hbm, last_hi),
                (last_lo_hbm, last_lo),
            )
        )
    ]
    loads[0].wait()
    loads[1].wait()
    samples = cell_ref.shape[1]
    start = jnp.broadcast_to(
        cell_ref[...] - block * GRID_DEV + (TILE - (TAPS // 2 - 1)), (TILE, samples)
    )
    row = lax.broadcasted_iota(jnp.int32, (TILE, samples), 0)
    phase = start & (TILE - 1)
    tap = (row - phase) & (TILE - 1)
    shifted = tap.astype(jnp.float32) - float(TAPS // 2 - 1) - frac_ref[...]
    values = jnp.exp(-sharpness * (shifted * shifted))
    values = jnp.where(tap < TAPS, values, 0.0).astype(jnp.bfloat16)
    tile_of = (lax.shift_right_logical(start, 4) + jnp.where(row < phase, 1, 0)).astype(
        jnp.float32
    )
    edge = jnp.where(row < TILE // 2, float(GRID_DEV // TILE + 1), 0.0)
    nothing = jnp.zeros_like(values)
    edge_window = jnp.where(tile_of == edge, values.astype(jnp.float32), 0.0).astype(jnp.bfloat16)
    tile_of = tile_of.astype(jnp.bfloat16)

    def build(chunk):
        for i in range(CHUNK // TILE):
            q = chunk * (CHUNK // TILE) + i
            window[q * TILE : (q + 1) * TILE, :] = jnp.where(
                tile_of == jnp.bfloat16(q + 1), values, nothing
            )

    across = (((1,), (1,)), ((), ()))

    def rows():
        return strength[...].reshape(2 * strength.shape[2], samples)

    def gather(chunk):
        return lax.dot_general(
            rows(),
            window[chunk * CHUNK : (chunk + 1) * CHUNK, :],
            across,
            preferred_element_type=jnp.float32,
        )

    def round_out(chunk, total):
        channels = total.shape[0] // 2
        real = total[:channels].reshape(BLOCKS, 8, CHUNK)
        imag = total[channels:].reshape(BLOCKS, 8, CHUNK)
        upper = lax.broadcasted_iota(jnp.int32, real.shape, 1) < 4
        outgoing[0, :, chunk] = jnp.where(upper, real, pltpu.roll(imag, 4, 1)).astype(jnp.bfloat16)
        outgoing[1, :, chunk] = jnp.where(upper, pltpu.roll(real, 4, 1), imag).astype(jnp.bfloat16)

    own_plane = (block >> 1) & 7
    offsets = [
        (((block >> 4) + (inner >> 1)) & 1) * 16 + ((block + inner) & 1) for inner in range(4)
    ]

    def send(half, begin, count, far=0):
        landing = (first, second)[half]
        dst = landing.at[group // 2, block % 4, group % 2, pl.ds(begin, count)]

        def one(step, carry):
            position = plane(step, own_plane, far)
            for inner in range(4):
                target = offsets[inner] + 2 * position
                src = outgoing.at[half, target, pl.ds(begin, count)]
                remote = pltpu.make_async_remote_copy(
                    src_ref=src,
                    dst_ref=dst,
                    send_sem=send_sem,
                    recv_sem=recv_sem.at[half],
                    device_id=(target, frame),
                    device_id_type=MESH,
                )
                if inner:
                    remote.start()
                    continue
                own = jnp.logical_and(position == own_plane, frame == group)

                @pl.when(jnp.logical_not(own))
                def _():
                    remote.start()

                @pl.when(own)
                def _():
                    pltpu.make_async_copy(src, dst, recv_sem.at[half]).start()

            return carry

        lax.fori_loop(0, 8, one, 0)

    build(1)
    total = None
    for piece in range(PIECES):
        loads[2 + piece].wait()
        span = slice(piece * PIECE, (piece + 1) * PIECE)
        part = lax.dot_general(
            strength[:, :, :, span].reshape(2 * strength.shape[2], PIECE),
            window[CHUNK : 2 * CHUNK, span],
            across,
            preferred_element_type=jnp.float32,
        )
        total = part if total is None else total + part
    round_out(1, total)
    pl.semaphore_wait(barrier, 34)
    send(0, 1, 1)
    for table in tables:
        table.start()
    halo[...] = lax.dot_general(edge_window, rows(), across, preferred_element_type=jnp.float32)
    to_right = pltpu.make_async_remote_copy(
        src_ref=halo.at[0:8],
        dst_ref=halo_in.at[0:8],
        send_sem=halo_send_sem,
        recv_sem=halo_recv_sem,
        device_id=(right, group),
        device_id_type=MESH,
    )
    to_left = pltpu.make_async_remote_copy(
        src_ref=halo.at[8:16],
        dst_ref=halo_in.at[120:128],
        send_sem=halo_send_sem,
        recv_sem=halo_recv_sem,
        device_id=(left, group),
        device_id_type=MESH,
    )
    to_right.start()
    to_left.start()
    build(2)
    round_out(2, gather(2))
    send(0, 2, 1)
    build(0)
    partial[0] = gather(0)
    build(3)
    partial[1] = gather(3)
    halo_in[8:120, :] = jnp.zeros((112, halo_in.shape[1]), jnp.float32)

    pltpu.make_async_copy(halo, halo_in.at[0:16], halo_recv_sem).wait()
    beyond = halo_in[...].T
    lane = lax.broadcasted_iota(jnp.int32, beyond.shape, 1)
    none = jnp.zeros((beyond.shape[0], CHUNK - 128), jnp.float32)
    round_out(
        0, partial[0] + jnp.concatenate([jnp.where(lane < 8, beyond, 0.0), none], axis=1)
    )
    send(0, 0, 1, 1)
    round_out(
        3, partial[1] + jnp.concatenate([none, jnp.where(lane >= 120, beyond, 0.0)], axis=1)
    )
    send(0, 3, 1, 1)
    send(1, 0, 4)

    for table in tables:
        table.wait()
    pltpu.make_async_copy(outgoing.at[0], first, recv_sem.at[0]).wait()

    def one_pair(pair, carry):
        data = first[pair].reshape(256, 256)
        store_pair(
            spectra, pair, transform_pair(data, first_hi, first_lo, turns, last_hi, last_lo)
        )
        return carry

    lax.fori_loop(0, PAIRS, one_pair, 0)

    pltpu.make_async_copy(halo, halo_in.at[0:16], halo_send_sem).wait()

    @pl.when(frame == group)
    def _():
        pltpu.make_async_copy(outgoing.at[:, 0:31], outgoing.at[:, 0:31], send_sem).wait()

    @pl.when(frame != group)
    def _():
        pltpu.make_async_copy(outgoing, outgoing, send_sem).wait()

    pltpu.make_async_copy(outgoing.at[1], second, recv_sem.at[1]).wait()


def spread(strengths, sample_cell, sample_frac, tables):
    channels, samples = strengths.shape[2], strengths.shape[3]
    rows = 2 * channels
    half_shape = (PAIRS, 4, 2, CHUNKS, *MESSAGE)
    inputs = (
        strengths,
        sample_cell.reshape(1, samples),
        sample_frac.reshape(1, samples),
        *tables,
    )
    return pl.pallas_call(
        spread_kernel,
        out_shape=(
            jax.ShapeDtypeStruct(half_shape, jnp.bfloat16),
            jax.ShapeDtypeStruct((PAIRS, 2, 2, 4, FFT_LO, FFT_HI), jnp.float32),
            *(jax.ShapeDtypeStruct(table.shape, table.dtype) for table in tables),
        ),
        in_specs=[pl.BlockSpec(memory_space=pltpu.HBM)] * len(inputs),
        out_specs=(pl.BlockSpec(memory_space=pltpu.VMEM),) * (2 + len(tables)),
        scratch_shapes=[
            pltpu.VMEM((1, samples), jnp.int32),
            pltpu.VMEM((1, samples), jnp.float32),
            pltpu.VMEM(strengths.shape, jnp.bfloat16),
            pltpu.VMEM((GRID_DEV, samples), jnp.bfloat16),
            pltpu.VMEM((HALVES, BLOCKS, CHUNKS, *MESSAGE), jnp.bfloat16),
            pltpu.VMEM(half_shape, jnp.bfloat16),
            pltpu.VMEM((2, rows, CHUNK), jnp.float32),
            pltpu.VMEM((16, rows), jnp.float32),
            pltpu.VMEM((128, rows), jnp.float32),
            pltpu.SemaphoreType.DMA((2 + PIECES,)),
            pltpu.SemaphoreType.DMA((5,)),
            pltpu.SemaphoreType.DMA,
            pltpu.SemaphoreType.DMA((2,)),
            pltpu.SemaphoreType.DMA,
            pltpu.SemaphoreType.DMA,
        ],
        compiler_params=pltpu.CompilerParams(
            collective_id=0, has_side_effects=True, vmem_limit_bytes=48 * 1024 * 1024
        ),
    )(*(pltpu.with_memory_space_constraint(x, pltpu.HBM) for x in inputs))


def split_bf16(table):
    high = table.astype(jnp.bfloat16)
    low = (table - high.astype(np.float64)).astype(jnp.bfloat16)
    return high, low


def transform_tables():
    digit = np.arange(16)
    angle = 2.0 * math.pi * (digit[:, None] * digit[None, :] % 16) / 16
    cos, sin = np.cos(angle), np.sin(angle)
    group, channel = np.eye(2), np.eye(4)

    def entry(part):
        return np.einsum("atm,gh,cd->gcathmd", part.reshape(16, 4, 4), group, channel)

    first = np.zeros((2, 2, 4, 16, 4, 2, 4, 2, 4))
    first[0, ..., 0, :] = entry(cos)
    first[0, ..., 1, :] = entry(sin)
    first[1, ..., 0, :] = entry(-sin)
    first[1, ..., 1, :] = entry(cos)
    first = first.reshape(256, 256)

    n = np.arange(FFT_HI)
    half_turn = 2.0 * math.pi * digit[:, None] / FFT_LO * np.ones((1, FFT_HI))
    turn = 2.0 * math.pi * np.arange(FFT_LO)[:, None] * n[None, :] / FFTLEN
    turns = np.stack(
        [
            np.cos(half_turn),
            np.sin(half_turn),
            np.cos(turn[:16]),
            np.sin(turn[:16]),
            np.cos(turn[16:]),
            np.sin(turn[16:]),
        ]
    ).astype(np.float32)

    angle = 2.0 * math.pi * (n[:, None] * n[None, :] % FFT_HI) / FFT_HI
    cos, sin = np.cos(angle), np.sin(angle)
    last = np.block([[cos, -sin], [sin, cos]]) / math.sqrt(FFTLEN)
    return (*split_bf16(first), turns, *split_bf16(last))


def finish_kernel(
    data_ref, done, first_hi, first_lo, turns, last_hi, last_lo, out_hbm, *scratch
):
    *outs, done_sem, sem = scratch

    def place(src, half, pair, semaphore):
        return pltpu.make_async_copy(
            src, out_hbm.at[:, pl.ds(2 * pair, 2), pl.ds(4 * half, 4), 0], semaphore
        )

    early = [place(done.at[pair], 0, pair, done_sem) for pair in range(PAIRS)]
    late = [place(outs[pair].at[0], 1, pair, sem) for pair in range(PAIRS)]
    for copy in early:
        copy.start()
    results = [
        transform_pair(
            data_ref[pair].reshape(256, 256), first_hi, first_lo, turns, last_hi, last_lo
        )
        for pair in range(PAIRS)
    ]
    for pair in range(PAIRS):
        store_pair(outs[pair], 0, results[pair])
        if pair > 0:
            late[pair - 1].start()
    late[PAIRS - 1].start()
    for copy in early + late:
        copy.wait()


def finish(second, spectra, tables):
    return pl.pallas_call(
        finish_kernel,
        out_shape=jax.ShapeDtypeStruct((2, 8, 8, 1, FFT_LO, FFT_HI), jnp.float32),
        in_specs=[pl.BlockSpec(memory_space=pltpu.VMEM)] * 7,
        out_specs=pl.BlockSpec(memory_space=pltpu.HBM),
        scratch_shapes=[
            *(pltpu.VMEM((1, 2, 2, 4, FFT_LO, FFT_HI), jnp.float32),) * PAIRS,
            pltpu.SemaphoreType.DMA,
            pltpu.SemaphoreType.DMA,
        ],
        compiler_params=pltpu.CompilerParams(vmem_limit_bytes=32 * 1024 * 1024),
    )(second, spectra, *tables)


def shards(strengths, sample_cell, sample_frac):
    tables = tuple(jnp.asarray(table) for table in transform_tables())
    second, spectra, *tables = spread(strengths, sample_cell, sample_frac, tables)
    return finish(second, spectra, tables)


def solution(mesh):
    placed = (P(None, "freq", None, "tm"), P("tm"), P("tm"))
    return jax.shard_map(
        shards,
        mesh=mesh,
        in_specs=placed,
        out_specs=P(None, None, "tm", "freq", None, None),
        check_vma=False,
    )
```
